32 devices in a mesh: gy: 2 (over y), gx: 4 (over z), gz: 4 (over x, core).
Axes of the slice: x: 2, y: 2, z: 4, core: 2. Of those that a mesh axis runs over, the one named last changes fastest.
Arguments:
- potential_warmth: float32 [32, 256, 512], P('gz', 'gy', 'gx'), may hold values from -6 to 6
- saltiness_anomaly: float32 [32, 256, 512], P('gz', 'gy', 'gx'), may hold values from -6 to 6
- squared_brunt_vaisala: float32 [32, 256, 512], P('gz', 'gy', 'gx'), may hold values from 0.5 to 2
- cross_density_mixing: float32 [32, 256, 512], P('gz', 'gy', 'gx'), may hold values from 0.1 to 10
- along_neutral_mixing: float32 [32, 256, 512], P('gz', 'gy', 'gx'), may hold values from 0.04 to 0.2
- layer_depth_mixing: float32 [32, 256, 512], P('gz', 'gy', 'gx'), may hold values from 0.04 to 0.2
- seawater_profile_flag: int32 [256, 512], P('gy', 'gx'), may hold values 0 or 1
- submerged_layer_total: int32 [256, 512], P('gy', 'gx'), may hold values from 1 to 32
Outputs:
- temperature_new: float32 [32, 256, 512], P('gz', 'gy', 'gx')
- salinity_new: float32 [32, 256, 512], P('gz', 'gy', 'gx')
The draws below stay inside these ranges and needn't reach their ends.
All inputs are finite; a program needn't handle non-finite values. No bound on the sum of `seawater_profile_flag` on one device may be relied on, other than what follows from the above.
Results may differ from the reference program's by a relative error of at most 0.00002.
Values sent between devices are 32-bit elements; how exact they have to be, the bound alone decides.
A program may use at most 128 MiB of HBM per device.

```python
import math
import jax
import jax.numpy as jnp
from jax import lax

EAST_WEST_SPAN = 512
NORTH_SOUTH_SPAN = 256
DEPTH_STRATA = 32


def place_ends(drawn, key, least, largest):
    dims = drawn.shape
    index_at = [jax.random.randint(jax.random.fold_in(key, axis), (), 0, dims[axis]) for axis in range(len(dims))]
    drawn = drawn.at[tuple(index_at)].set(least)
    longest = dims.index(max(dims))
    index_at[longest] = (index_at[longest] + 1) % dims[longest]
    return drawn.at[tuple(index_at)].set(largest)


def block_levels(stream_key, shape, pieces, least, high):
    def one(position, parts):
        steps = jax.random.uniform(jax.random.fold_in(jax.random.fold_in(stream_key, 6), position), (parts,), jnp.float32, least / len(pieces), high / len(pieces))
        return jnp.repeat(jnp.exp(steps), shape[position] // parts).reshape((-1,) + (1,) * (len(shape) - position - 1))

    factor_of = one(*pieces[0])
    for cut in pieces[1:]:
        factor_of = factor_of * one(*cut)
    return factor_of


def gaussian(rng, shape, scale, reach, shards=(), held_as=jnp.bfloat16):
    entries = scale * jax.random.normal(rng, shape, jnp.float32)
    if shards:
        entries = entries * block_levels(rng, shape, shards, -0.22, 0.18)
    return jnp.clip(entries, -reach, reach).astype(held_as)


def setup_inputs(seed: int = 0) -> dict:
    streams_of = jax.random.split(jax.random.key(seed), 9)
    potential_warmth = gaussian(streams_of[0], (DEPTH_STRATA, NORTH_SOUTH_SPAN, EAST_WEST_SPAN), 1.0, 6.0, ((0, 4), (1, 2), (2, 4)), jnp.float32)
    saltiness_anomaly = gaussian(streams_of[1], (DEPTH_STRATA, NORTH_SOUTH_SPAN, EAST_WEST_SPAN), 1.0, 6.0, ((0, 4), (1, 2), (2, 4)), jnp.float32)
    squared_brunt_vaisala = jnp.clip(jnp.exp(math.log(2.0) - 1.3862944 * jax.random.uniform(streams_of[2], (DEPTH_STRATA, NORTH_SOUTH_SPAN, EAST_WEST_SPAN), jnp.float32) ** block_levels(streams_of[2], (DEPTH_STRATA, NORTH_SOUTH_SPAN, EAST_WEST_SPAN), ((0, 4), (1, 2), (2, 4)), -0.2, 0.2)), 0.5, 2.0)
    cross_density_mixing = jnp.clip(jnp.exp(math.log(10.0) - 4.6051702 * jax.random.uniform(streams_of[3], (DEPTH_STRATA, NORTH_SOUTH_SPAN, EAST_WEST_SPAN), jnp.float32) ** block_levels(streams_of[3], (DEPTH_STRATA, NORTH_SOUTH_SPAN, EAST_WEST_SPAN), ((0, 4), (1, 2), (2, 4)), -0.2, 0.2)), 0.1, 10.0)
    along_neutral_mixing = jnp.clip(jnp.exp(math.log(0.2) - 1.609438 * jax.random.uniform(streams_of[4], (DEPTH_STRATA, NORTH_SOUTH_SPAN, EAST_WEST_SPAN), jnp.float32) ** block_levels(streams_of[4], (DEPTH_STRATA, NORTH_SOUTH_SPAN, EAST_WEST_SPAN), ((0, 4), (1, 2), (2, 4)), -0.2, 0.2)), 0.04, 0.2)
    layer_depth_mixing = jnp.clip(jnp.exp(math.log(0.2) - 1.609438 * jax.random.uniform(streams_of[5], (DEPTH_STRATA, NORTH_SOUTH_SPAN, EAST_WEST_SPAN), jnp.float32) ** block_levels(streams_of[5], (DEPTH_STRATA, NORTH_SOUTH_SPAN, EAST_WEST_SPAN), ((0, 4), (1, 2), (2, 4)), -0.2, 0.2)), 0.04, 0.2)
    seawater_profile_flag = place_ends((jax.random.randint(streams_of[6], (NORTH_SOUTH_SPAN, EAST_WEST_SPAN), 0, 5) < 4).astype(jnp.int32), jax.random.fold_in(streams_of[6], 1), 0, 1)
    submerged_layer_total = place_ends(jax.random.randint(streams_of[7], (NORTH_SOUTH_SPAN, EAST_WEST_SPAN), 1, DEPTH_STRATA + 1), jax.random.fold_in(streams_of[7], 1), 1, DEPTH_STRATA).astype(jnp.int32)
    return dict(potential_warmth=potential_warmth, saltiness_anomaly=saltiness_anomaly, squared_brunt_vaisala=squared_brunt_vaisala, cross_density_mixing=cross_density_mixing, along_neutral_mixing=along_neutral_mixing, layer_depth_mixing=layer_depth_mixing, seawater_profile_flag=seawater_profile_flag, submerged_layer_total=submerged_layer_total)


step_dt = 1.0


def explicit_part(extended, cross_density_mixing):
    tracer = extended[0:2]
    density_lift_array = extended[2]
    stratum = extended[3]
    seawater_volume_flag = extended[4]
    redi_coef = extended[5]
    bolus_coef = extended[6]
    wet_x = seawater_volume_flag[:, :, 1:] * seawater_volume_flag[:, :, :-1]
    grad_bx = (density_lift_array[:, :, 1:] - density_lift_array[:, :, :-1]) * wet_x
    slope_x = -grad_bx / (0.5 * (stratum[:, :, 1:] + stratum[:, :, :-1]) + jnp.abs(grad_bx) + 1.0 - wet_x)
    diff_x = (tracer[..., 1:] - tracer[..., :-1]) * wet_x
    wet_y = seawater_volume_flag[:, 1:, :] * seawater_volume_flag[:, :-1, :]
    grad_by = (density_lift_array[:, 1:, :] - density_lift_array[:, :-1, :]) * wet_y
    slope_y = -grad_by / (0.5 * (stratum[:, 1:, :] + stratum[:, :-1, :]) + jnp.abs(grad_by) + 1.0 - wet_y)
    diff_y = (tracer[:, :, 1:, :] - tracer[:, :, :-1, :]) * wet_y
    wet_z = seawater_volume_flag[1:] * seawater_volume_flag[:-1]
    diff_z = (tracer[:, 1:] - tracer[:, :-1]) * wet_z
    centre_z = 0.5 * (diff_z[:, 1:] + diff_z[:, :-1])
    redi_x = 0.5 * (redi_coef[1:-1, 1:-1, 1:] + redi_coef[1:-1, 1:-1, :-1])
    bolus_x = 0.5 * (bolus_coef[1:-1, 1:-1, 1:] + bolus_coef[1:-1, 1:-1, :-1])
    flux_x = -(redi_x * diff_x[:, 1:-1, 1:-1, :] + (redi_x - bolus_x) * slope_x[1:-1, 1:-1, :] * 0.5 * (centre_z[:, :, 1:-1, 1:] + centre_z[:, :, 1:-1, :-1]))
    redi_y = 0.5 * (redi_coef[1:-1, 1:, 1:-1] + redi_coef[1:-1, :-1, 1:-1])
    bolus_y = 0.5 * (bolus_coef[1:-1, 1:, 1:-1] + bolus_coef[1:-1, :-1, 1:-1])
    flux_y = -(redi_y * diff_y[:, 1:-1, :, 1:-1] + (redi_y - bolus_y) * slope_y[1:-1, :, 1:-1] * 0.5 * (centre_z[:, :, 1:, 1:-1] + centre_z[:, :, :-1, 1:-1]))
    slope_cx = 0.5 * (slope_x[:, 1:-1, 1:] + slope_x[:, 1:-1, :-1])
    grad_cx = 0.5 * (diff_x[:, :, 1:-1, 1:] + diff_x[:, :, 1:-1, :-1])
    slope_cy = 0.5 * (slope_y[:, 1:, 1:-1] + slope_y[:, :-1, 1:-1])
    grad_cy = 0.5 * (diff_y[:, :, 1:, 1:-1] + diff_y[:, :, :-1, 1:-1])
    cross = slope_cx * grad_cx + slope_cy * grad_cy
    total_coef = (redi_coef + bolus_coef)[:, 1:-1, 1:-1]
    flux_z = -0.5 * (total_coef[1:] * cross[:, 1:] + total_coef[:-1] * cross[:, :-1]) * wet_z[:, 1:-1, 1:-1]
    tendency = -(flux_x[..., 1:] - flux_x[..., :-1]) - (flux_y[:, :, 1:, :] - flux_y[:, :, :-1, :]) - (flux_z[:, 1:] - flux_z[:, :-1])
    inner_wet = seawater_volume_flag[1:-1, 1:-1, 1:-1]
    fresh = (tracer[:, 1:-1, 1:-1, 1:-1] + step_dt * tendency) * inner_wet
    square_slope = slope_cx * slope_cx + slope_cy * slope_cy
    couple = (cross_density_mixing + 0.5 * (redi_coef[1:-1, 1:-1, 1:-1] * square_slope[1:-1] + redi_coef[2:, 1:-1, 1:-1] * square_slope[2:])) * wet_z[1:, 1:-1, 1:-1]
    return fresh, couple


def solve_columns(couple, fresh):
    lower = -step_dt * jnp.concatenate([jnp.zeros_like(couple[:1]), couple[:-1]], axis=0)
    upper = -step_dt * couple
    middle = 1.0 - lower - upper
    right = jnp.moveaxis(fresh, 1, 0)

    def forward(carry, items):
        prev_c, prev_d = carry
        low, mid, upp, rhs = items
        denom = mid - low * prev_c
        next_c = upp / denom
        next_d = (rhs - low * prev_d) / denom
        return (next_c, next_d), (next_c, next_d)

    start = (jnp.zeros(couple.shape[1:], jnp.float32), jnp.zeros(right.shape[1:], jnp.float32))
    _, (coef_c, coef_d) = lax.scan(forward, start, (lower, middle, upper, right))

    def backward(later, items):
        cur_c, cur_d = items
        value = cur_d - cur_c * later
        return value, value

    _, values = lax.scan(backward, jnp.zeros(right.shape[1:], jnp.float32), (coef_c, coef_d), reverse=True)
    return jnp.moveaxis(values, 0, 1)


def reference(potential_warmth, saltiness_anomaly, squared_brunt_vaisala, cross_density_mixing, along_neutral_mixing, layer_depth_mixing, seawater_profile_flag, submerged_layer_total):
    levels = jnp.arange(DEPTH_STRATA, dtype=jnp.int32)[:, None, None]
    seawater_volume_flag = ((seawater_profile_flag[None] == 1) & (levels < submerged_layer_total[None])).astype(jnp.float32)
    density_lift_array = jnp.cumsum(squared_brunt_vaisala, axis=0)
    joined_solutes = jnp.stack([potential_warmth, saltiness_anomaly, density_lift_array, squared_brunt_vaisala, seawater_volume_flag, along_neutral_mixing, layer_depth_mixing])
    joined_solutes = jnp.pad(joined_solutes, ((0, 0), (0, 0), (0, 0), (1, 1)), mode="wrap")
    extended = jnp.pad(joined_solutes, ((0, 0), (1, 1), (1, 1), (0, 0)))
    fresh, couple = explicit_part(extended, cross_density_mixing)
    solved = solve_columns(couple, fresh)
    return solved[0], solved[1]
```

```python
import functools

import jax
import jax.numpy as jnp
from jax import lax
from jax.experimental import pallas as pl
from jax.experimental.pallas import tpu as pltpu
from jax.sharding import PartitionSpec as P

MESH = pl.DeviceIdType.MESH
CHUNK = 16
PAD = 8
ORIG, LATE = 5, 3
(Z_UP, Z_DOWN, V_DOWN, PRE, XA_R, XA_L, YA_L, YA_R, XB_R, XB_L, YB_L, YB_R, PROD_UP, PROD_DOWN, CHAIN, MIDDLE, BACK) = range(17)


def kernel(
    t_in, s_in, n_in, v_in, i_in, g_in, flag_in, count_in,
    t_out, s_out,
    ext, late, depth, zh, vext, flag, count, psend, pre,
    xa, xa_got, xb, xb_got, ya, ya_got, yb, yb_got, comb_a, comb_b,
    prod, rhs, cpl, elim, ch_out, ch_in, mid_in, last, solved, back_in,
    local_sem, send_sem, recv_sem,
):
    L, R, C = t_in.shape
    gx, gy, gz = (lax.axis_index(a) for a in ("gx", "gy", "gz"))
    nx, ny, nz = (lax.axis_size(a) for a in ("gx", "gy", "gz"))
    right, left = lax.rem(gx + 1, nx), lax.rem(gx + nx - 1, nx)
    later, earlier = lax.rem(gy + 1, ny), lax.rem(gy + ny - 1, ny)
    below, above = lax.rem(gz + 1, nz), lax.rem(gz + nz - 1, nz)
    inner = pl.ds(PAD, R)
    f32 = jnp.float32

    def load(number, src, dst):
        return pltpu.make_async_copy(src, dst, local_sem.at[number])

    loads = [
        load(0, n_in, ext.at[:, 2, inner, :]),
        load(1, t_in, ext.at[:, 0, inner, :]),
        load(2, s_in, ext.at[:, 1, inner, :]),
        load(3, i_in, ext.at[:, 3, inner, :]),
        load(4, g_in, ext.at[:, 4, inner, :]),
        load(5, flag_in, flag),
        load(6, count_in, count),
        load(7, v_in, vext.at[pl.ds(1, L)]),
    ]
    for item in loads:
        item.start()

    barrier = pltpu.get_barrier_semaphore()
    for target in ({"gx": right}, {"gx": left}, {"gy": later}, {"gy": earlier}, {"gz": below}, {"gz": above}):
        pl.semaphore_signal(barrier, inc=1, device_id=target, device_id_type=MESH)
    pl.semaphore_wait(barrier, 6)

    def remote(number, src, dst, target):
        return pltpu.make_async_remote_copy(
            src_ref=src, dst_ref=dst, send_sem=send_sem.at[number], recv_sem=recv_sem.at[number],
            device_id=target, device_id_type=MESH,
        )

    has_above, has_below = gz > 0, gz < nz - 1
    has_earlier, has_later = gy > 0, gy < ny - 1
    always = None

    def when(condition, action):
        if condition is None:
            action()
        else:
            pl.when(condition)(action)

    sends = []

    def send(condition, item):
        when(condition, item.start)
        sends.append((condition, item))

    z_up = remote(Z_UP, ext.at[0, pl.ds(0, 2), inner, :], zh.at[1], {"gz": above})
    z_down = remote(Z_DOWN, ext.at[L - 1, pl.ds(0, 2), inner, :], zh.at[0], {"gz": below})
    v_down = remote(V_DOWN, vext.at[L], vext.at[0], {"gz": below})
    p_down = remote(PRE, psend, pre, {"gz": below})

    loads[0].wait()

    def column_sum(step, carry):
        rows = pl.ds(pl.multiple_of(step * CHUNK, PAD), CHUNK)
        rows_e = pl.ds(pl.multiple_of(PAD + step * CHUNK, PAD), CHUNK)
        total = ext[0, 2, rows_e, :]
        for k in range(1, L):
            total = total + ext[k, 2, rows_e, :]
        psend[rows, :] = total
        return carry

    chunks = R // CHUNK
    lax.fori_loop(0, chunks, column_sum, 0)

    @pl.when(gz == 0)
    def _():
        pre[...] = jnp.zeros_like(pre)

    @pl.when(gz == 0)
    def _():
        p_down.start()

    sends.append((has_below, p_down))
    loads[1].wait()
    loads[2].wait()
    send(has_above, z_up)
    send(has_below, z_down)

    loads[5].wait()
    loads[6].wait()
    depth[inner, :] = jnp.where(flag[...] == 1, count[...], 0).astype(f32)

    @pl.when(gz > 0)
    def _():
        p_down.wait_recv()

        @pl.when(has_below)
        def _():
            psend[...] = psend[...] + pre[...]
            p_down.start()

    loads[3].wait()
    loads[4].wait()

    def pack(source, fields, extra, out):
        def body(step, carry):
            rows = pl.ds(pl.multiple_of(step * CHUNK, PAD), CHUNK)
            rows_e = pl.ds(pl.multiple_of(PAD + step * CHUNK, PAD), CHUNK)
            pair = lax.broadcasted_iota(jnp.int32, (CHUNK, C), 1) // 2
            acc = jnp.zeros((CHUNK, C), f32)
            for m in range(L * fields + extra):
                slab = depth[rows_e, :] if m == L * fields else source[m // fields, m % fields, rows_e, :]
                acc = jnp.where(pair == m, pltpu.roll(slab, 2 * m + 1, 1), acc)
            out[rows, :] = acc
            return carry

        lax.fori_loop(0, chunks, body, 0)

    def pack_rows(source, fields, extra, out):
        for m in range(L * fields + extra):
            for side, row in ((0, PAD), (1, PAD + R - 1)):
                if m == L * fields:
                    out[side, pl.ds(m, 1), :] = depth[pl.ds(row, 1), :]
                else:
                    out[side, pl.ds(m, 1), :] = source[m // fields, m % fields, pl.ds(row, 1), :]

    def unpack_rows(source, fields, extra, got):
        for m in range(L * fields + extra):
            for side, row in ((0, PAD - 1), (1, PAD + R)):
                value = got[side, pl.ds(m, 1), :]
                if m == L * fields:
                    depth[pl.ds(row, 1), :] = value
                else:
                    source[m // fields, m % fields, pl.ds(row, 1), :] = value

    def combine(got, out):
        lane = lax.broadcasted_iota(jnp.int32, (R, C), 1)
        out[...] = jnp.where(lane % 2 == 0, pltpu.roll(got[1], C - 1, 1), pltpu.roll(got[0], 1, 1))

    pack_rows(ext, ORIG, 1, ya)
    pack(ext, ORIG, 1, xa)
    ya_l = remote(YA_L, ya.at[0], ya_got.at[1], {"gy": earlier})
    ya_r = remote(YA_R, ya.at[1], ya_got.at[0], {"gy": later})
    xa_r = remote(XA_R, xa, xa_got.at[0], {"gx": right})
    xa_l = remote(XA_L, xa, xa_got.at[1], {"gx": left})
    send(has_earlier, ya_l)
    send(has_later, ya_r)
    send(always, xa_r)
    send(always, xa_l)
    loads[7].wait()
    send(has_below, v_down)

    @pl.when(gz == 0)
    def _():
        zh[0] = jnp.zeros_like(zh[0])
        vext[0] = jnp.zeros_like(vext[0])
        prod[0] = jnp.zeros_like(prod[0])

    @pl.when(gz == nz - 1)
    def _():
        zh[1] = jnp.zeros_like(zh[1])
        prod[L + 1] = jnp.zeros_like(prod[L + 1])

    @pl.when(gy == 0)
    def _():
        ya_got[0] = jnp.zeros_like(ya_got[0])
        yb_got[0] = jnp.zeros_like(yb_got[0])

    @pl.when(gy == ny - 1)
    def _():
        ya_got[1] = jnp.zeros_like(ya_got[1])
        yb_got[1] = jnp.zeros_like(yb_got[1])

    when(has_above, z_down.wait_recv)
    when(has_below, z_up.wait_recv)

    def wet_at(deep, k):
        level = gz * L + k
        return ((deep > level.astype(f32)) & (level >= 0)).astype(f32)

    def vertical(step, carry):
        rows = pl.ds(pl.multiple_of(step * CHUNK, PAD), CHUNK)
        rows_e = pl.ds(pl.multiple_of(PAD + step * CHUNK, PAD), CHUNK)
        deep = depth[rows_e, :]
        total = pre[rows, :]
        w_here = wet_at(deep, 0)
        gate = wet_at(deep, -1) * w_here
        cells = [ext[0, c, rows_e, :] for c in range(2)]
        over = [(cells[c] - zh[0, c, rows, :]) * gate for c in range(2)]
        for k in range(L):
            total = total + ext[k, 2, rows_e, :]
            late[k, 0, rows_e, :] = total
            w_next = wet_at(deep, k + 1)
            gate = w_here * w_next
            for c in range(2):
                following = ext[k + 1, c, rows_e, :] if k + 1 < L else zh[1, c, rows, :]
                under = (following - cells[c]) * gate
                late[k, 1 + c, rows_e, :] = 0.5 * (under + over[c])
                cells[c], over[c] = following, under
            w_here = w_next
        return carry

    lax.fori_loop(0, chunks, vertical, 0)
    pack_rows(late, LATE, 0, yb)
    pack(late, LATE, 0, xb)
    yb_l = remote(YB_L, yb.at[0], yb_got.at[1], {"gy": earlier})
    yb_r = remote(YB_R, yb.at[1], yb_got.at[0], {"gy": later})
    xb_r = remote(XB_R, xb, xb_got.at[0], {"gx": right})
    xb_l = remote(XB_L, xb, xb_got.at[1], {"gx": left})
    send(has_earlier, yb_l)
    send(has_later, yb_r)
    send(always, xb_r)
    send(always, xb_l)

    when(has_earlier, ya_r.wait_recv)
    when(has_later, ya_l.wait_recv)
    unpack_rows(ext, ORIG, 1, ya_got)
    xa_r.wait_recv()
    xa_l.wait_recv()
    combine(xa_got, comb_a)
    when(has_earlier, yb_r.wait_recv)
    when(has_later, yb_l.wait_recv)
    unpack_rows(late, LATE, 0, yb_got)
    xb_r.wait_recv()
    xb_l.wait_recv()
    combine(xb_got, comb_b)

    def face(a, b):
        wet = a["w"] * b["w"]
        lift = (b["B"] - a["B"]) * wet
        slope = -lift / (0.5 * (a["N"] + b["N"]) + jnp.abs(lift) + 1.0 - wet)
        along = 0.5 * (a["I"] + b["I"])
        skew = (along - 0.5 * (a["G"] + b["G"])) * slope * 0.5
        steps, fluxes = [], []
        for c, g in (("T", "gT"), ("S", "gS")):
            step = (b[c] - a[c]) * wet
            steps.append(step)
            fluxes.append(-(along * step + skew * (a[g] + b[g])))
        return slope, steps, fluxes

    names_a, names_b = ("T", "S", "N", "I", "G"), ("B", "gT", "gS")

    def level_body(k):
        for chunk in range(chunks):
            r0 = chunk * CHUNK
            rows = pl.ds(r0, CHUNK)
            lane = lax.broadcasted_iota(jnp.int32, (CHUNK, C), 1)
            packed_a, packed_b = comb_a[rows, :], comb_b[rows, :]

            def cell(shift):
                rows_e = pl.ds(PAD + r0 + shift, CHUNK)
                out = {name: ext[k, f, rows_e, :] for f, name in enumerate(names_a)}
                out.update({name: late[k, f, rows_e, :] for f, name in enumerate(names_b)})
                out["D"] = depth[rows_e, :]
                return out

            here, north, south = cell(0), cell(-1), cell(1)
            east, west = {}, {}
            for name, value in here.items():
                if name == "D":
                    edge = pltpu.roll(packed_a, C - 1 - 2 * ORIG * L, 1)
                elif name in names_a:
                    edge = pltpu.roll(packed_a, C - 1 - 2 * (k * ORIG + names_a.index(name)), 1)
                else:
                    edge = pltpu.roll(packed_b, C - 1 - 2 * (k * LATE + names_b.index(name)), 1)
                east[name] = jnp.where(lane == C - 1, edge, pltpu.roll(value, C - 1, 1))
                west[name] = jnp.where(lane == 0, edge, pltpu.roll(value, 1, 1))
            for item in (here, north, south, east, west):
                item["w"] = wet_at(item["D"], k)
            slope_w, step_w, flux_w = face(west, here)
            slope_e, step_e, flux_e = face(here, east)
            slope_n, step_n, flux_n = face(north, here)
            slope_s, step_s, flux_s = face(here, south)
            sx, sy = 0.5 * (slope_w + slope_e), 0.5 * (slope_n + slope_s)
            both = here["I"] + here["G"]
            for c, name in enumerate(("T", "S")):
                cross = sx * (0.5 * (step_w[c] + step_e[c])) + sy * (0.5 * (step_n[c] + step_s[c]))
                prod[k + 1, c, rows, :] = both * cross
                rhs[k, c, rows, :] = here[name] - (flux_e[c] - flux_w[c]) - (flux_s[c] - flux_n[c])
            prod[k + 1, 2, rows, :] = here["I"] * (sx * sx + sy * sy)

    def ends(step, carry):
        level_body(step * (L - 1))
        return carry

    def middles(k, carry):
        level_body(k)
        return carry

    lax.fori_loop(0, 2, ends, 0)
    prod_up = remote(PROD_UP, prod.at[1], prod.at[L + 1], {"gz": above})
    prod_down = remote(PROD_DOWN, prod.at[L], prod.at[0], {"gz": below})
    send(has_above, prod_up)
    send(has_below, prod_down)
    lax.fori_loop(1, L - 1, middles, 0)
    when(has_above, v_down.wait_recv)
    when(has_above, prod_down.wait_recv)
    when(has_below, prod_up.wait_recv)

    def assemble(step, carry):
        rows = pl.ds(pl.multiple_of(step * CHUNK, PAD), CHUNK)
        rows_e = pl.ds(pl.multiple_of(PAD + step * CHUNK, PAD), CHUNK)
        deep = depth[rows_e, :]
        wets = [wet_at(deep, k) for k in range(-1, L + 1)]
        prods = [prod[0, c, rows, :] for c in range(3)]
        flux = [None, None]
        for k in range(-1, L):
            gate = wets[k + 1] * wets[k + 2]
            nexts = [prod[k + 2, c, rows, :] for c in range(3)]
            for c in range(2):
                under = -0.5 * (nexts[c] + prods[c]) * gate
                if k >= 0:
                    rhs[k, c, rows, :] = (rhs[k, c, rows, :] - (under - flux[c])) * wets[k + 1]
                flux[c] = under
            cpl[k + 1, rows, :] = (vext[k + 1, rows, :] + 0.5 * (prods[2] + nexts[2])) * gate
            prods = nexts
        return carry

    lax.fori_loop(0, chunks, assemble, 0)

    upper = gz < nz // 2
    at_end = (gz == 0) | (gz == nz - 1)
    in_middle = (gz == nz // 2 - 1) | (gz == nz // 2)
    flip = jnp.where(upper, 0, 1)
    onward = jnp.where(upper, below, above)
    backward = jnp.where(upper, above, below)

    def level_at(j):
        return j + flip * (L - 1 - 2 * j)

    chain = remote(CHAIN, ch_out, ch_in, {"gz": onward})
    middle = remote(MIDDLE, ch_out, mid_in, {"gz": onward})
    back = remote(BACK, solved.at[level_at(0)], back_in, {"gz": backward})

    @pl.when(at_end)
    def _():
        ch_in[...] = jnp.zeros_like(ch_in)

    when(jnp.logical_not(at_end), chain.wait_recv)

    def eliminate(step, carry):
        rows = pl.ds(pl.multiple_of(step * CHUNK, PAD), CHUNK)
        weight, sums = ch_in[0, rows, :], [ch_in[1 + c, rows, :] for c in range(2)]
        for j in range(L):
            k = level_at(j)
            link = cpl[k + 1 - flip, rows, :]
            held = 1.0 + weight
            share = 1.0 / (held + link)
            factor = link * share
            right_side = [rhs[k, c, rows, :] + sums[c] for c in range(2)]
            if j == L - 1:
                last[0, rows, :] = held
                for c in range(2):
                    last[1 + c, rows, :] = right_side[c]
            weight = factor * held
            elim[j, 0, rows, :] = factor
            for c in range(2):
                elim[j, 1 + c, rows, :] = right_side[c] * share
                sums[c] = right_side[c] * factor
        ch_out[0, rows, :] = weight
        for c in range(2):
            ch_out[1 + c, rows, :] = sums[c]
        return carry

    lax.fori_loop(0, chunks, eliminate, 0)
    not_middle = jnp.logical_not(in_middle)
    not_end = jnp.logical_not(at_end)
    send(not_middle, chain)
    send(in_middle, middle)
    k_last = level_at(L - 1)

    @pl.when(in_middle)
    def _():
        middle.wait_recv()
        share = 1.0 / (last[0] + mid_in[0])
        for c in range(2):
            solved[k_last, c] = (last[1 + c] + mid_in[1 + c]) * share

    @pl.when(not_middle)
    def _():
        back.wait_recv()
        for c in range(2):
            solved[k_last, c] = elim[L - 1, 1 + c] + elim[L - 1, 0] * back_in[c]

    def substitute(step, carry):
        rows = pl.ds(pl.multiple_of(step * CHUNK, PAD), CHUNK)
        values = [solved[k_last, c, rows, :] for c in range(2)]
        for j in range(L - 2, -1, -1):
            k = level_at(j)
            factor = elim[j, 0, rows, :]
            for c in range(2):
                values[c] = elim[j, 1 + c, rows, :] + factor * values[c]
                solved[k, c, rows, :] = values[c]
        return carry

    lax.fori_loop(0, chunks, substitute, 0)
    send(not_end, back)
    stores = [load(8, solved.at[:, 0], t_out), load(9, solved.at[:, 1], s_out)]
    for item in stores:
        item.start()
    for item in stores:
        item.wait()
    for condition, item in sends:
        when(condition, item.wait_send)


def shards(*blocks):
    L, R, C = blocks[0].shape
    f32 = jnp.float32
    na, nb = L * ORIG + 1, L * LATE
    na_pad, nb_pad = -(-na // 8) * 8, -(-nb // 8) * 8
    assert 2 * na <= C and 2 * nb <= C and R % CHUNK == 0
    vmem = pltpu.VMEM
    slab = (R, C)
    scratch = [
        vmem((L, ORIG, R + 2 * PAD, C), f32),
        vmem((L, LATE, R + 2 * PAD, C), f32),
        vmem((R + 2 * PAD, C), f32),
        vmem((2, 2) + slab, f32),
        vmem((L + 1,) + slab, f32),
        vmem(slab, jnp.int32),
        vmem(slab, jnp.int32),
        vmem(slab, f32),
        vmem(slab, f32),
        vmem(slab, f32),
        vmem((2,) + slab, f32),
        vmem(slab, f32),
        vmem((2,) + slab, f32),
        vmem((2, na_pad, C), f32),
        vmem((2, na_pad, C), f32),
        vmem((2, nb_pad, C), f32),
        vmem((2, nb_pad, C), f32),
        vmem(slab, f32),
        vmem(slab, f32),
        vmem((L + 2, 3) + slab, f32),
        vmem((L, 2) + slab, f32),
        vmem((L + 1,) + slab, f32),
        vmem((L, 3) + slab, f32),
        vmem((3,) + slab, f32),
        vmem((3,) + slab, f32),
        vmem((3,) + slab, f32),
        vmem((3,) + slab, f32),
        vmem((L, 2) + slab, f32),
        vmem((2,) + slab, f32),
        pltpu.SemaphoreType.DMA((10,)),
        pltpu.SemaphoreType.DMA((17,)),
        pltpu.SemaphoreType.DMA((17,)),
    ]
    return pl.pallas_call(
        kernel,
        out_shape=[jax.ShapeDtypeStruct((L, R, C), f32)] * 2,
        in_specs=[pl.BlockSpec(memory_space=pl.ANY)] * 8,
        out_specs=[pl.BlockSpec(memory_space=pl.ANY)] * 2,
        scratch_shapes=scratch,
        compiler_params=pltpu.CompilerParams(
            collective_id=0, has_side_effects=True, vmem_limit_bytes=48 * 1024 * 1024
        ),
    )(*blocks)


def solution(mesh):
    field, flat = P("gz", "gy", "gx"), P("gy", "gx")
    return jax.shard_map(
        shards,
        mesh=mesh,
        in_specs=(field,) * 6 + (flat,) * 2,
        out_specs=(field, field),
        check_vma=False,
    )
```

```python
import functools

import jax
import jax.numpy as jnp
from jax import lax
from jax.experimental import pallas as pl
from jax.experimental.pallas import tpu as pltpu
from jax.sharding import PartitionSpec as P

MESH = pl.DeviceIdType.MESH
CHUNK = 16
PAD = 8
ORIG, LATE = 5, 3
(Z_UP, Z_DOWN, V_DOWN, PRE, XA_R, XA_L, YA_L, YA_R, XB_R, XB_L, YB_L, YB_R, PROD_UP, PROD_DOWN, CHAIN, MIDDLE, BACK) = range(17)


def kernel(
    t_in, s_in, n_in, v_in, i_in, g_in, flag_in, count_in,
    t_out, s_out,
    ext, late, depth, zh, vext, flag, count, psend, pre,
    xa, xa_got, xb, xb_got, ya, ya_got, yb, yb_got, comb_a, comb_b,
    prod, rhs, cpl, elim, ch_out, ch_in, mid_in, last, solved, back_in,
    local_sem, send_sem, recv_sem,
):
    L, R, C = t_in.shape
    gx, gy, gz = (lax.axis_index(a) for a in ("gx", "gy", "gz"))
    nx, ny, nz = (lax.axis_size(a) for a in ("gx", "gy", "gz"))
    right, left = lax.rem(gx + 1, nx), lax.rem(gx + nx - 1, nx)
    later, earlier = lax.rem(gy + 1, ny), lax.rem(gy + ny - 1, ny)
    below, above = lax.rem(gz + 1, nz), lax.rem(gz + nz - 1, nz)
    inner = pl.ds(PAD, R)
    f32 = jnp.float32

    def load(number, src, dst):
        return pltpu.make_async_copy(src, dst, local_sem.at[number])

    loads = [
        load(0, n_in, ext.at[:, 2, inner, :]),
        load(1, t_in, ext.at[:, 0, inner, :]),
        load(2, s_in, ext.at[:, 1, inner, :]),
        load(3, i_in, ext.at[:, 3, inner, :]),
        load(4, g_in, ext.at[:, 4, inner, :]),
        load(5, flag_in, flag),
        load(6, count_in, count),
        load(7, v_in, vext.at[pl.ds(1, L)]),
    ]
    for item in loads:
        item.start()

    barrier = pltpu.get_barrier_semaphore()
    for target in ({"gx": right}, {"gx": left}, {"gy": later}, {"gy": earlier}, {"gz": below}, {"gz": above}):
        pl.semaphore_signal(barrier, inc=1, device_id=target, device_id_type=MESH)

    def remote(number, src, dst, target):
        return pltpu.make_async_remote_copy(
            src_ref=src, dst_ref=dst, send_sem=send_sem.at[number], recv_sem=recv_sem.at[number],
            device_id=target, device_id_type=MESH,
        )

    has_above, has_below = gz > 0, gz < nz - 1
    has_earlier, has_later = gy > 0, gy < ny - 1
    always = None

    def when(condition, action):
        if condition is None:
            action()
        else:
            pl.when(condition)(action)

    sends = []

    def send(condition, item):
        when(condition, item.start)
        sends.append((condition, item))

    z_up = remote(Z_UP, ext.at[0, pl.ds(0, 2), inner, :], zh.at[1], {"gz": above})
    z_down = remote(Z_DOWN, ext.at[L - 1, pl.ds(0, 2), inner, :], zh.at[0], {"gz": below})
    v_down = remote(V_DOWN, vext.at[L], vext.at[0], {"gz": below})
    p_down = remote(PRE, psend, pre, {"gz": below})

    loads[0].wait()

    def column_sum(step, carry):
        rows = pl.ds(pl.multiple_of(step * CHUNK, PAD), CHUNK)
        rows_e = pl.ds(pl.multiple_of(PAD + step * CHUNK, PAD), CHUNK)
        total = ext[0, 2, rows_e, :]
        for k in range(1, L):
            total = total + ext[k, 2, rows_e, :]
        psend[rows, :] = total
        return carry

    chunks = R // CHUNK
    lax.fori_loop(0, chunks, column_sum, 0)

    @pl.when(gz == 0)
    def _():
        pre[...] = jnp.zeros_like(pre)

    pl.semaphore_wait(barrier, 6)

    @pl.when(gz == 0)
    def _():
        p_down.start()

    sends.append((has_below, p_down))
    loads[1].wait()
    loads[2].wait()
    send(has_above, z_up)
    send(has_below, z_down)

    loads[5].wait()
    loads[6].wait()
    depth[inner, :] = jnp.where(flag[...] == 1, count[...], 0).astype(f32)

    @pl.when(has_above & has_below)
    def _():
        p_down.wait_recv()
        psend[...] = psend[...] + pre[...]
        p_down.start()

    loads[3].wait()
    loads[4].wait()

    def pack(source, fields, extra, out):
        def body(step, carry):
            rows = pl.ds(pl.multiple_of(step * CHUNK, PAD), CHUNK)
            rows_e = pl.ds(pl.multiple_of(PAD + step * CHUNK, PAD), CHUNK)
            pair = lax.broadcasted_iota(jnp.int32, (CHUNK, C), 1) // 2
            acc = jnp.zeros((CHUNK, C), f32)
            for m in range(L * fields + extra):
                slab = depth[rows_e, :] if m == L * fields else source[m // fields, m % fields, rows_e, :]
                acc = jnp.where(pair == m, pltpu.roll(slab, 2 * m + 1, 1), acc)
            out[rows, :] = acc
            return carry

        lax.fori_loop(0, chunks, body, 0)

    def pack_rows(source, fields, extra, out):
        for m in range(L * fields + extra):
            for side, row in ((0, PAD), (1, PAD + R - 1)):
                if m == L * fields:
                    out[side, pl.ds(m, 1), :] = depth[pl.ds(row, 1), :]
                else:
                    out[side, pl.ds(m, 1), :] = source[m // fields, m % fields, pl.ds(row, 1), :]

    def unpack_rows(source, fields, extra, got):
        for m in range(L * fields + extra):
            for side, row in ((0, PAD - 1), (1, PAD + R)):
                value = got[side, pl.ds(m, 1), :]
                if m == L * fields:
                    depth[pl.ds(row, 1), :] = value
                else:
                    source[m // fields, m % fields, pl.ds(row, 1), :] = value

    def combine(got, out):
        lane = lax.broadcasted_iota(jnp.int32, (R, C), 1)
        out[...] = jnp.where(lane % 2 == 0, pltpu.roll(got[1], C - 1, 1), pltpu.roll(got[0], 1, 1))

    pack_rows(ext, ORIG, 1, ya)
    pack(ext, ORIG, 1, xa)
    ya_l = remote(YA_L, ya.at[0], ya_got.at[1], {"gy": earlier})
    ya_r = remote(YA_R, ya.at[1], ya_got.at[0], {"gy": later})
    xa_r = remote(XA_R, xa, xa_got.at[0], {"gx": right})
    xa_l = remote(XA_L, xa, xa_got.at[1], {"gx": left})
    send(has_earlier, ya_l)
    send(has_later, ya_r)
    send(always, xa_r)
    send(always, xa_l)
    loads[7].wait()
    send(has_below, v_down)

    @pl.when(gz == 0)
    def _():
        zh[0] = jnp.zeros_like(zh[0])
        vext[0] = jnp.zeros_like(vext[0])
        prod[0] = jnp.zeros_like(prod[0])

    @pl.when(gz == nz - 1)
    def _():
        zh[1] = jnp.zeros_like(zh[1])
        prod[L + 1] = jnp.zeros_like(prod[L + 1])

    @pl.when(gy == 0)
    def _():
        ya_got[0] = jnp.zeros_like(ya_got[0])
        yb_got[0] = jnp.zeros_like(yb_got[0])

    @pl.when(gy == ny - 1)
    def _():
        ya_got[1] = jnp.zeros_like(ya_got[1])
        yb_got[1] = jnp.zeros_like(yb_got[1])

    when(has_above, z_down.wait_recv)
    when(has_below, z_up.wait_recv)
    when(jnp.logical_not(has_below), p_down.wait_recv)

    def wet_at(deep, k):
        level = gz * L + k
        return ((deep > level.astype(f32)) & (level >= 0)).astype(f32)

    def vertical(step, carry):
        rows = pl.ds(pl.multiple_of(step * CHUNK, PAD), CHUNK)
        rows_e = pl.ds(pl.multiple_of(PAD + step * CHUNK, PAD), CHUNK)
        deep = depth[rows_e, :]
        total = pre[rows, :]
        w_here = wet_at(deep, 0)
        gate = wet_at(deep, -1) * w_here
        cells = [ext[0, c, rows_e, :] for c in range(2)]
        over = [(cells[c] - zh[0, c, rows, :]) * gate for c in range(2)]
        for k in range(L):
            total = total + ext[k, 2, rows_e, :]
            late[k, 0, rows_e, :] = total
            w_next = wet_at(deep, k + 1)
            gate = w_here * w_next
            for c in range(2):
                following = ext[k + 1, c, rows_e, :] if k + 1 < L else zh[1, c, rows, :]
                under = (following - cells[c]) * gate
                late[k, 1 + c, rows_e, :] = 0.5 * (under + over[c])
                cells[c], over[c] = following, under
            w_here = w_next
        return carry

    lax.fori_loop(0, chunks, vertical, 0)
    pack_rows(late, LATE, 0, yb)
    pack(late, LATE, 0, xb)
    yb_l = remote(YB_L, yb.at[0], yb_got.at[1], {"gy": earlier})
    yb_r = remote(YB_R, yb.at[1], yb_got.at[0], {"gy": later})
    xb_r = remote(XB_R, xb, xb_got.at[0], {"gx": right})
    xb_l = remote(XB_L, xb, xb_got.at[1], {"gx": left})
    send(has_earlier, yb_l)
    send(has_later, yb_r)
    send(always, xb_r)
    send(always, xb_l)

    when(has_earlier, ya_r.wait_recv)
    when(has_later, ya_l.wait_recv)
    unpack_rows(ext, ORIG, 1, ya_got)
    xa_r.wait_recv()
    xa_l.wait_recv()
    combine(xa_got, comb_a)
    when(has_earlier, yb_r.wait_recv)
    when(has_later, yb_l.wait_recv)
    unpack_rows(late, LATE, 0, yb_got)
    xb_r.wait_recv()
    xb_l.wait_recv()
    combine(xb_got, comb_b)

    def face(a, b):
        wet = a["w"] * b["w"]
        lift = (b["B"] - a["B"]) * wet
        slope = -lift / (0.5 * (a["N"] + b["N"]) + jnp.abs(lift) + 1.0 - wet)
        along = 0.5 * (a["I"] + b["I"])
        skew = (along - 0.5 * (a["G"] + b["G"])) * slope * 0.5
        steps, fluxes = [], []
        for c, g in (("T", "gT"), ("S", "gS")):
            step = (b[c] - a[c]) * wet
            steps.append(step)
            fluxes.append(-(along * step + skew * (a[g] + b[g])))
        return slope, steps, fluxes

    names_a, names_b = ("T", "S", "N", "I", "G"), ("B", "gT", "gS")

    def level_body(k):
        for chunk in range(chunks):
            r0 = chunk * CHUNK
            rows = pl.ds(r0, CHUNK)
            lane = lax.broadcasted_iota(jnp.int32, (CHUNK, C), 1)
            packed_a, packed_b = comb_a[rows, :], comb_b[rows, :]

            def cell(shift):
                rows_e = pl.ds(PAD + r0 + shift, CHUNK)
                out = {name: ext[k, f, rows_e, :] for f, name in enumerate(names_a)}
                out.update({name: late[k, f, rows_e, :] for f, name in enumerate(names_b)})
                out["D"] = depth[rows_e, :]
                return out

            here, north, south = cell(0), cell(-1), cell(1)
            east, west = {}, {}
            for name, value in here.items():
                if name == "D":
                    edge = pltpu.roll(packed_a, C - 1 - 2 * ORIG * L, 1)
                elif name in names_a:
                    edge = pltpu.roll(packed_a, C - 1 - 2 * (k * ORIG + names_a.index(name)), 1)
                else:
                    edge = pltpu.roll(packed_b, C - 1 - 2 * (k * LATE + names_b.index(name)), 1)
                east[name] = jnp.where(lane == C - 1, edge, pltpu.roll(value, C - 1, 1))
                west[name] = jnp.where(lane == 0, edge, pltpu.roll(value, 1, 1))
            for item in (here, north, south, east, west):
                item["w"] = wet_at(item["D"], k)
            slope_w, step_w, flux_w = face(west, here)
            slope_e, step_e, flux_e = face(here, east)
            slope_n, step_n, flux_n = face(north, here)
            slope_s, step_s, flux_s = face(here, south)
            sx, sy = 0.5 * (slope_w + slope_e), 0.5 * (slope_n + slope_s)
            both = here["I"] + here["G"]
            for c, name in enumerate(("T", "S")):
                cross = sx * (0.5 * (step_w[c] + step_e[c])) + sy * (0.5 * (step_n[c] + step_s[c]))
                prod[k + 1, c, rows, :] = both * cross
                rhs[k, c, rows, :] = here[name] - (flux_e[c] - flux_w[c]) - (flux_s[c] - flux_n[c])
            prod[k + 1, 2, rows, :] = here["I"] * (sx * sx + sy * sy)

    def ends(step, carry):
        level_body(step * (L - 1))
        return carry

    def middles(k, carry):
        level_body(k)
        return carry

    lax.fori_loop(0, 2, ends, 0)
    prod_up = remote(PROD_UP, prod.at[1], prod.at[L + 1], {"gz": above})
    prod_down = remote(PROD_DOWN, prod.at[L], prod.at[0], {"gz": below})
    send(has_above, prod_up)
    send(has_below, prod_down)
    lax.fori_loop(1, L - 1, middles, 0)
    when(has_above, v_down.wait_recv)
    when(has_above, prod_down.wait_recv)
    when(has_below, prod_up.wait_recv)

    def assemble(step, carry):
        rows = pl.ds(pl.multiple_of(step * CHUNK, PAD), CHUNK)
        rows_e = pl.ds(pl.multiple_of(PAD + step * CHUNK, PAD), CHUNK)
        deep = depth[rows_e, :]
        wets = [wet_at(deep, k) for k in range(-1, L + 1)]
        prods = [prod[0, c, rows, :] for c in range(3)]
        flux = [None, None]
        for k in range(-1, L):
            gate = wets[k + 1] * wets[k + 2]
            nexts = [prod[k + 2, c, rows, :] for c in range(3)]
            for c in range(2):
                under = -0.5 * (nexts[c] + prods[c]) * gate
                if k >= 0:
                    rhs[k, c, rows, :] = (rhs[k, c, rows, :] - (under - flux[c])) * wets[k + 1]
                flux[c] = under
            cpl[k + 1, rows, :] = (vext[k + 1, rows, :] + 0.5 * (prods[2] + nexts[2])) * gate
            prods = nexts
        return carry

    lax.fori_loop(0, chunks, assemble, 0)

    upper = gz < nz // 2
    at_end = (gz == 0) | (gz == nz - 1)
    in_middle = (gz == nz // 2 - 1) | (gz == nz // 2)
    flip = jnp.where(upper, 0, 1)
    onward = jnp.where(upper, below, above)
    backward = jnp.where(upper, above, below)

    def level_at(j):
        return j + flip * (L - 1 - 2 * j)

    chain = remote(CHAIN, ch_out, ch_in, {"gz": onward})
    middle = remote(MIDDLE, ch_out, mid_in, {"gz": onward})
    back = remote(BACK, solved.at[level_at(0)], back_in, {"gz": backward})

    @pl.when(at_end)
    def _():
        ch_in[...] = jnp.zeros_like(ch_in)

    when(jnp.logical_not(at_end), chain.wait_recv)

    def eliminate(step, carry):
        rows = pl.ds(pl.multiple_of(step * CHUNK, PAD), CHUNK)
        weight, sums = ch_in[0, rows, :], [ch_in[1 + c, rows, :] for c in range(2)]
        for j in range(L):
            k = level_at(j)
            link = cpl[k + 1 - flip, rows, :]
            held = 1.0 + weight
            share = 1.0 / (held + link)
            factor = link * share
            right_side = [rhs[k, c, rows, :] + sums[c] for c in range(2)]
            if j == L - 1:
                last[0, rows, :] = held
                for c in range(2):
                    last[1 + c, rows, :] = right_side[c]
            weight = factor * held
            elim[j, 0, rows, :] = factor
            for c in range(2):
                elim[j, 1 + c, rows, :] = right_side[c] * share
                sums[c] = right_side[c] * factor
        ch_out[0, rows, :] = weight
        for c in range(2):
            ch_out[1 + c, rows, :] = sums[c]
        return carry

    lax.fori_loop(0, chunks, eliminate, 0)
    not_middle = jnp.logical_not(in_middle)
    not_end = jnp.logical_not(at_end)
    send(not_middle, chain)
    send(in_middle, middle)
    k_last = level_at(L - 1)

    @pl.when(in_middle)
    def _():
        middle.wait_recv()
        share = 1.0 / (last[0] + mid_in[0])
        for c in range(2):
            solved[k_last, c] = (last[1 + c] + mid_in[1 + c]) * share

    @pl.when(not_middle)
    def _():
        back.wait_recv()
        for c in range(2):
            solved[k_last, c] = elim[L - 1, 1 + c] + elim[L - 1, 0] * back_in[c]

    def substitute(step, carry):
        rows = pl.ds(pl.multiple_of(step * CHUNK, PAD), CHUNK)
        values = [solved[k_last, c, rows, :] for c in range(2)]
        for j in range(L - 2, -1, -1):
            k = level_at(j)
            factor = elim[j, 0, rows, :]
            for c in range(2):
                values[c] = elim[j, 1 + c, rows, :] + factor * values[c]
                solved[k, c, rows, :] = values[c]
        return carry

    lax.fori_loop(0, chunks, substitute, 0)
    send(not_end, back)
    stores = [load(8, solved.at[:, 0], t_out), load(9, solved.at[:, 1], s_out)]
    for item in stores:
        item.start()
    for item in stores:
        item.wait()
    for condition, item in sends:
        when(condition, item.wait_send)


def shards(*blocks):
    L, R, C = blocks[0].shape
    f32 = jnp.float32
    na, nb = L * ORIG + 1, L * LATE
    na_pad, nb_pad = -(-na // 8) * 8, -(-nb // 8) * 8
    assert 2 * na <= C and 2 * nb <= C and R % CHUNK == 0
    vmem = pltpu.VMEM
    slab = (R, C)
    scratch = [
        vmem((L, ORIG, R + 2 * PAD, C), f32),
        vmem((L, LATE, R + 2 * PAD, C), f32),
        vmem((R + 2 * PAD, C), f32),
        vmem((2, 2) + slab, f32),
        vmem((L + 1,) + slab, f32),
        vmem(slab, jnp.int32),
        vmem(slab, jnp.int32),
        vmem(slab, f32),
        vmem(slab, f32),
        vmem(slab, f32),
        vmem((2,) + slab, f32),
        vmem(slab, f32),
        vmem((2,) + slab, f32),
        vmem((2, na_pad, C), f32),
        vmem((2, na_pad, C), f32),
        vmem((2, nb_pad, C), f32),
        vmem((2, nb_pad, C), f32),
        vmem(slab, f32),
        vmem(slab, f32),
        vmem((L + 2, 3) + slab, f32),
        vmem((L, 2) + slab, f32),
        vmem((L + 1,) + slab, f32),
        vmem((L, 3) + slab, f32),
        vmem((3,) + slab, f32),
        vmem((3,) + slab, f32),
        vmem((3,) + slab, f32),
        vmem((3,) + slab, f32),
        vmem((L, 2) + slab, f32),
        vmem((2,) + slab, f32),
        pltpu.SemaphoreType.DMA((10,)),
        pltpu.SemaphoreType.DMA((17,)),
        pltpu.SemaphoreType.DMA((17,)),
    ]
    return pl.pallas_call(
        kernel,
        out_shape=[jax.ShapeDtypeStruct((L, R, C), f32)] * 2,
        in_specs=[pl.BlockSpec(memory_space=pl.ANY)] * 8,
        out_specs=[pl.BlockSpec(memory_space=pl.ANY)] * 2,
        scratch_shapes=scratch,
        compiler_params=pltpu.CompilerParams(
            collective_id=0, has_side_effects=True, vmem_limit_bytes=67043328
        ),
    )(*blocks)


def solution(mesh):
    field, flat = P("gz", "gy", "gx"), P("gy", "gx")
    return jax.shard_map(
        shards,
        mesh=mesh,
        in_specs=(field,) * 6 + (flat,) * 2,
        out_specs=(field, field),
        check_vma=False,
    )
```
